16 devices in a mesh: dp: 4 (over y, z, core), tp: 4 (over x).
Axes of the slice: x: 4, y: 2, z: 1, core: 2. Of those that a mesh axis runs over, the one named last changes fastest.
The devices are a block of a 4x4x4 slice.
Arguments:
- x: bfloat16 [2560, 7168], P(('dp', 'tp')), parts along dimension 0
- dy: bfloat16 [2560, 7168], P(('dp', 'tp')), parts along dimension 0
- pre: bfloat16 [2560, 28672], P('dp', 'tp'), parts along dimension 0
- w_in: bfloat16 [7168, 28672], P(None, 'tp')
- w_down: bfloat16 [28672, 7168], P('tp')
Outputs:
- output 1: bfloat16 [2560, 7168], P(('dp', 'tp')), parts along dimension 0
- output 2: bfloat16 [28672, 28672], P('dp', 'tp'), parts along dimension 0
- output 3: bfloat16 [114688, 7168], P(('dp', 'tp')), parts along dimension 0
There are 4 independent parts. The reference program is written for one: setup_inputs(seed, part) draws one part's arguments, and reference() takes and returns one part's arrays. A program takes and returns all parts, laid end to end along the dimension named above; an argument that names none is the same for every part.
All inputs are finite; a program needn't handle non-finite values.
Results may differ from the reference program's by a relative error of at most 0.012.
Values are sent between devices in bfloat16 or wider.
A program may use at most 1.5 GiB of HBM per device.

```python
import jax
import jax.numpy as jnp

ROWS = 640
D = 7168
FF = 28672


def act(pre):
    return jax.nn.gelu(pre)


def setup_inputs(seed: int = 0, part: int = 0) -> dict:
    kx, ky, ka, ki, kd = jax.random.split(jax.random.key(seed), 5)
    kx, ky, ka = (jax.random.fold_in(k, part) for k in (kx, ky, ka))
    drawn = {
        "x": jax.random.normal(kx, (ROWS, D), jnp.float32),
        "dy": jax.random.normal(ky, (ROWS, D), jnp.float32),
        "pre": jax.random.normal(ka, (ROWS, FF), jnp.float32),
        "w_in": jax.random.normal(ki, (D, FF), jnp.float32) * D**-0.5,
        "w_down": jax.random.normal(kd, (FF, D), jnp.float32) * FF**-0.5,
    }
    return {k: v.astype(jnp.bfloat16) for k, v in drawn.items()}


def reference(x, dy, pre, w_in, w_down):
    hidden, back = jax.vjp(act, pre.astype(jnp.float32))
    d_hidden = jnp.dot(dy, w_down.T, preferred_element_type=jnp.float32)
    d_pre = back(d_hidden)[0].astype(jnp.bfloat16)
    dx = jnp.dot(d_pre, w_in.T, preferred_element_type=jnp.float32)
    dw_in = jnp.dot(x.T, d_pre, preferred_element_type=jnp.float32)
    dw_down = jnp.dot(hidden.astype(jnp.bfloat16).T, dy, preferred_element_type=jnp.float32)
    return tuple(g.astype(jnp.bfloat16) for g in (dx, dw_in, dw_down))
```

```python
import functools

import jax
import jax.numpy as jnp
from jax import lax
from jax.experimental import pallas as pl
from jax.experimental.pallas import tpu as pltpu
from jax.sharding import PartitionSpec as P

VMEM_LIMIT = 60 * 1024 * 1024


def act(pre):
    return jax.nn.gelu(pre)


def params(n=1):
    return pltpu.CompilerParams(
        dimension_semantics=("arbitrary",) * n, vmem_limit_bytes=VMEM_LIMIT
    )


def whole(shape):
    return pl.BlockSpec(shape, lambda *i: (0,) * len(shape), pipeline_mode=pl.Buffered(1))


def gelu_kernel(pre_ref, hidden_ref, slope_ref):
    hidden, back = jax.vjp(act, pre_ref[...].astype(jnp.float32))
    slope_ref[...] = back(jnp.ones_like(hidden))[0]
    hidden_ref[...] = hidden.astype(jnp.bfloat16).T


def gelu_pass(pre, tile):
    rows, cols = pre.shape
    return pl.pallas_call(
        gelu_kernel,
        grid=(cols // tile,),
        in_specs=[pl.BlockSpec((rows, tile), lambda i: (0, i))],
        out_specs=[
            pl.BlockSpec((tile, rows), lambda i: (i, 0)),
            pl.BlockSpec((rows, tile), lambda i: (0, i)),
        ],
        out_shape=[
            jax.ShapeDtypeStruct((cols, rows), jnp.bfloat16),
            jax.ShapeDtypeStruct((rows, cols), jnp.float32),
        ],
        compiler_params=params(),
        cost_estimate=pl.CostEstimate(
            flops=30 * rows * cols, bytes_accessed=8 * rows * cols, transcendentals=rows * cols
        ),
        name="gelu",
    )(pre)


def down_kernel(hidden_ref, dy_ref, *refs):
    out_ref = refs[-1]
    out_ref[...] = jnp.dot(
        hidden_ref[...], dy_ref[...], preferred_element_type=jnp.float32
    ).astype(out_ref.dtype)


def down_pass(hidden_t, dy, into, start, cols, tile):
    m, k = hidden_t.shape
    n = dy.shape[1]
    at = start // n
    args, specs, alias = [hidden_t, dy], [
        pl.BlockSpec((tile, k), lambda i: (i, 0)),
        whole((k, n)),
    ], {}
    if into is not None:
        args.append(into)
        specs.append(pl.BlockSpec(memory_space=pl.ANY))
        alias = {2: 0}
    return pl.pallas_call(
        down_kernel,
        grid=(m // tile,),
        in_specs=specs,
        out_specs=pl.BlockSpec((tile, n), lambda i: (i, at)),
        out_shape=jax.ShapeDtypeStruct((m, cols), jnp.bfloat16),
        input_output_aliases=alias,
        compiler_params=params(),
        cost_estimate=pl.CostEstimate(
            flops=2 * m * k * n, bytes_accessed=2 * (m * k + k * n + m * n), transcendentals=0
        ),
        name="dw_down",
    )(*args)


def pre_kernel(parts, *refs):
    dys, (w_ref, slope_ref, out_ref) = refs[:parts], refs[parts:]
    total, at = None, 0
    for dy_ref in dys:
        n = dy_ref.shape[1]
        term = lax.dot_general(
            dy_ref[...],
            w_ref[:, at : at + n],
            (((1,), (1,)), ((), ())),
            preferred_element_type=jnp.float32,
        )
        total = term if total is None else total + term
        at += n
    out_ref[...] = (total * slope_ref[...]).astype(out_ref.dtype)


def pre_pass(dys, w, slope, tile):
    rows = dys[0].shape[0]
    n, k = w.shape
    return pl.pallas_call(
        functools.partial(pre_kernel, len(dys)),
        grid=(n // tile,),
        in_specs=[whole(d.shape) for d in dys]
        + [
            pl.BlockSpec((tile, k), lambda i: (i, 0)),
            pl.BlockSpec((rows, tile), lambda i: (0, i)),
        ],
        out_specs=pl.BlockSpec((rows, tile), lambda i: (0, i)),
        out_shape=jax.ShapeDtypeStruct((rows, n), jnp.bfloat16),
        compiler_params=params(),
        cost_estimate=pl.CostEstimate(
            flops=2 * rows * n * k, bytes_accessed=2 * (rows * k + n * k + 3 * rows * n), transcendentals=0
        ),
        name="d_pre",
    )(*dys, w, slope)


def dx_kernel(d_ref, w_ref, out_ref):
    out_ref[...] = lax.dot_general(
        d_ref[...], w_ref[...], (((1,), (1,)), ((), ())), preferred_element_type=jnp.float32
    ).astype(out_ref.dtype)


def dx_pass(d_pre, w, start, cols, tile):
    rows, k = d_pre.shape
    at = start // tile
    return pl.pallas_call(
        dx_kernel,
        grid=(cols // tile,),
        in_specs=[whole((rows, k)), pl.BlockSpec((tile, k), lambda i: (i + at, 0))],
        out_specs=pl.BlockSpec((rows, tile), lambda i: (0, i)),
        out_shape=jax.ShapeDtypeStruct((rows, cols), jnp.bfloat16),
        compiler_params=params(),
        cost_estimate=pl.CostEstimate(
            flops=2 * rows * cols * k, bytes_accessed=2 * (rows * k + cols * k + rows * cols), transcendentals=0
        ),
        name="dx",
    )(d_pre, w)


def in_kernel(x_ref, d_ref, out_ref):
    out_ref[...] = lax.dot_general(
        x_ref[...], d_ref[...], (((0,), (0,)), ((), ())), preferred_element_type=jnp.float32
    ).astype(out_ref.dtype)


def in_pass(x, d_pre, tile):
    rows, m = x.shape
    n = d_pre.shape[1]
    return pl.pallas_call(
        in_kernel,
        grid=(m // tile,),
        in_specs=[pl.BlockSpec((rows, tile), lambda i: (0, i)), whole((rows, n))],
        out_specs=pl.BlockSpec((tile, n), lambda i: (i, 0)),
        out_shape=jax.ShapeDtypeStruct((m, n), jnp.bfloat16),
        compiler_params=params(),
        cost_estimate=pl.CostEstimate(
            flops=2 * rows * m * n, bytes_accessed=2 * (rows * m + rows * n + m * n), transcendentals=0
        ),
        name="dw_in",
    )(x, d_pre)


PARTS = 4
HALVES = 2


def solution(mesh):
    def step(x, dy, pre, w_in, w_down):
        d = dy.shape[1]
        part = d // PARTS
        gather = functools.partial(lax.all_gather, axis_name="tp", axis=0, tiled=True)
        dys = [gather(dy[:, i * part : (i + 1) * part]) for i in range(PARTS)]
        hidden_t, slope = gelu_pass(pre, 512)
        x, dys[-1] = lax.optimization_barrier((x, dys[-1]))
        x_all = gather(x)
        dw_down = None
        for i in range(PARTS):
            dw_down = down_pass(hidden_t, dys[i], dw_down, i * part, d, 1024)
        dys, dw_down = lax.optimization_barrier((dys, dw_down))
        d_pre = pre_pass(dys, w_down, slope, 512)
        half = w_in.shape[0] // HALVES
        dx = []
        for i in range(HALVES):
            term = dx_pass(d_pre, w_in, i * half, half, 512)
            dx.append(lax.psum_scatter(term, "tp", scatter_dimension=0, tiled=True))
        dw_in = in_pass(x_all, d_pre, 512)
        return jnp.concatenate(dx, axis=1), dw_in, dw_down

    return jax.shard_map(
        step,
        mesh=mesh,
        in_specs=(
            P(("dp", "tp"), None),
            P(("dp", "tp"), None),
            P("dp", "tp"),
            P(None, "tp"),
            P("tp", None),
        ),
        out_specs=(P(("dp", "tp"), None), P("dp", "tp"), P(("dp", "tp"), None)),
        check_vma=False,
    )
```

```python
import functools

import jax
import jax.numpy as jnp
from jax import lax
from jax.experimental import pallas as pl
from jax.experimental.pallas import tpu as pltpu
from jax.sharding import PartitionSpec as P

MESH = pl.DeviceIdType.MESH
VMEM_LIMIT = 60 * 1024 * 1024


CHUNKS = 7
BLOCKS = 4
STRIP = 256


def act(pre):
    return jax.nn.gelu(pre)


def whole(shape):
    return pl.BlockSpec(shape, lambda *i: (0,) * len(shape), pipeline_mode=pl.Buffered(1))


def front_kernel(
    dy_ref, pre_ref, w_ref, d_pre_ref, hidden_ref, all_ref,
    held, total, slope, pre_buf, hidden_buf, out_buf,
    send, recv, local, back, pre_sem, hidden_sem, out_sem,
):
    c, n = pl.program_id(0), pl.program_id(1)
    chunks, blocks = pl.num_programs(0), pl.num_programs(1)
    me = lax.axis_index("tp")
    right, left = lax.rem(me + 1, 4), lax.rem(me + 3, 4)
    rows, depth = dy_ref.shape[0], held.shape[2]
    half = rows // 2
    width = total.shape[2]
    per_block = width // STRIP
    strips = pre_ref.shape[1] // STRIP

    def columns(i, size):
        return pl.ds(pl.multiple_of(i * size, size), size)

    def rows_of(device, start, size):
        return pl.ds(pl.multiple_of(device * rows + start, 16), size)

    def load_own(i):
        return pltpu.make_async_copy(
            dy_ref.at[:, columns(i, depth)], held.at[i, rows_of(me, 0, rows), :], local.at[i]
        )

    def remote(kind, i, which, to):
        return pltpu.make_async_remote_copy(
            src_ref=held.at[i, which, :],
            dst_ref=held.at[i, which, :],
            send_sem=send.at[kind, i],
            recv_sem=recv.at[kind, i],
            device_id={"tp": to},
            device_id_type=MESH,
        )

    def own(i):
        which = rows_of(me, 0, rows)
        return remote(0, i, which, right), remote(1, i, which, left)

    def relay(i):
        return (
            remote(2, i, rows_of(left, 0, half), right),
            remote(3, i, rows_of(right, half, half), left),
        )

    def send_own(i):
        load_own(i).wait()
        for copy in own(i):
            copy.start()

    def pass_on(i):
        for arrived, onward in zip(own(i), relay(i)):
            arrived.wait_recv()
            onward.start()

    def load_pre(i, slot):
        return pltpu.make_async_copy(pre_ref.at[:, columns(i, STRIP)], pre_buf.at[slot], pre_sem.at[slot])

    def store_hidden(i, slot):
        return pltpu.make_async_copy(
            hidden_buf.at[slot], hidden_ref.at[columns(i, STRIP), :], hidden_sem.at[slot]
        )

    def gelu(i, _):
        slot = lax.rem(i, 2)
        load_pre(i, slot).wait()
        hidden, back_fn = jax.vjp(act, pre_buf[slot].astype(jnp.float32))
        at = (i // per_block, slice(None), columns(lax.rem(i, per_block), STRIP))
        slope[at] = back_fn(jnp.ones_like(hidden))[0]
        total[at] = jnp.zeros_like(hidden)

        @pl.when(i + 2 < strips)
        def _():
            load_pre(i + 2, slot).start()

        @pl.when(i >= 2)
        def _():
            store_hidden(i - 2, slot).wait()

        hidden_buf[slot] = hidden.astype(jnp.bfloat16).T
        store_hidden(i, slot).start()

    @pl.when((c == 0) & (n == 0))
    def _():
        for i in range(CHUNKS):
            load_own(i).start()
        for i in range(2):
            load_pre(i, i).start()
        barrier = pltpu.get_barrier_semaphore()
        for neighbour in (left, right):
            pl.semaphore_signal(barrier, inc=1, device_id={"tp": neighbour}, device_id_type=MESH)
        pl.semaphore_wait(barrier, 2)
        send_own(0)
        send_own(1)
        first, second = (strips * 9) // 16, (strips * 15) // 16
        lax.fori_loop(0, first, gelu, None)
        pass_on(0)
        send_own(2)
        lax.fori_loop(first, second, gelu, None)
        pass_on(1)
        send_own(3)
        lax.fori_loop(second, strips, gelu, None)
        for i in (strips - 2, strips - 1):
            store_hidden(i, i % 2).wait()

    @pl.when(n == 0)
    def _():
        for copy in relay(c):
            copy.wait_recv()
        pltpu.make_async_copy(held.at[c], all_ref.at[:, columns(c, depth)], back.at[c]).start()

    @pl.when((n == blocks - 1) & (c + 2 < chunks))
    def _():
        pass_on(c + 2)

        @pl.when(c + 4 < chunks)
        def _():
            send_own(c + 4)

    total[n] += lax.dot_general(
        held[c], w_ref[...], (((1,), (1,)), ((), ())), preferred_element_type=jnp.float32
    )

    def store_out(i):
        return pltpu.make_async_copy(out_buf, d_pre_ref.at[:, columns(i, width)], out_sem)

    @pl.when(c == chunks - 1)
    def _():
        @pl.when(n > 0)
        def _():
            store_out(n - 1).wait()

        out_buf[...] = (total[n] * slope[n]).astype(out_buf.dtype)
        store_out(n).start()

        @pl.when(n == blocks - 1)
        def _():
            store_out(n).wait()
            for i in range(CHUNKS):
                pltpu.make_async_copy(held.at[i], all_ref.at[:, columns(i, depth)], back.at[i]).wait()
                for copy in own(i) + relay(i):
                    copy.wait_send()


def front(dy, pre, w, size):
    assert size == 4
    rows, d = pre.shape[0], dy.shape[1]
    f = w.shape[0]
    depth, width = d // CHUNKS, f // BLOCKS
    anywhere = pl.BlockSpec(memory_space=pl.ANY)
    bf16 = jnp.bfloat16
    return pl.pallas_call(
        front_kernel,
        grid=(CHUNKS, BLOCKS),
        in_specs=[anywhere, anywhere, pl.BlockSpec((width, depth), lambda c, n: (n, c))],
        out_specs=[anywhere] * 3,
        out_shape=[
            jax.ShapeDtypeStruct((rows, f), bf16),
            jax.ShapeDtypeStruct((f, rows), bf16),
            jax.ShapeDtypeStruct((rows, d), bf16),
        ],
        scratch_shapes=[
            pltpu.VMEM((CHUNKS, rows, depth), bf16),
            pltpu.VMEM((BLOCKS, rows, width), jnp.float32),
            pltpu.VMEM((BLOCKS, rows, width), jnp.float32),
            pltpu.VMEM((2, rows, STRIP), bf16),
            pltpu.VMEM((2, STRIP, rows), bf16),
            pltpu.VMEM((rows, width), bf16),
            pltpu.SemaphoreType.DMA((4, CHUNKS)),
            pltpu.SemaphoreType.DMA((4, CHUNKS)),
            pltpu.SemaphoreType.DMA((CHUNKS,)),
            pltpu.SemaphoreType.DMA((CHUNKS,)),
            pltpu.SemaphoreType.DMA((2,)),
            pltpu.SemaphoreType.DMA((2,)),
            pltpu.SemaphoreType.DMA,
        ],
        compiler_params=pltpu.CompilerParams(
            dimension_semantics=("arbitrary",) * 2,
            vmem_limit_bytes=67043328,
            collective_id=0,
            has_side_effects=True,
        ),
        cost_estimate=pl.CostEstimate(
            flops=2 * rows * f * d, bytes_accessed=2 * (f * d + 4 * rows * d), transcendentals=rows * f
        ),
        name="front",
    )(dy, pre, w)


def product_kernel(a_ref, b_ref, out_ref):
    out_ref[...] = jnp.dot(a_ref[...], b_ref[...], preferred_element_type=jnp.float32).astype(out_ref.dtype)


def product_t_kernel(a_ref, b_ref, out_ref):
    out_ref[...] = lax.dot_general(
        a_ref[...], b_ref[...], (((0,), (0,)), ((), ())), preferred_element_type=jnp.float32
    ).astype(out_ref.dtype)


def weight_grad(a, b, tile, transposed, name):
    k, n = b.shape
    m = a.shape[1] if transposed else a.shape[0]
    spec = (
        pl.BlockSpec((k, tile), lambda i: (0, i)) if transposed else pl.BlockSpec((tile, k), lambda i: (i, 0))
    )
    return pl.pallas_call(
        product_t_kernel if transposed else product_kernel,
        grid=(m // tile,),
        in_specs=[spec, whole((k, n))],
        out_specs=pl.BlockSpec((tile, n), lambda i: (i, 0)),
        out_shape=jax.ShapeDtypeStruct((m, n), jnp.bfloat16),
        compiler_params=pltpu.CompilerParams(
            dimension_semantics=("arbitrary",), vmem_limit_bytes=VMEM_LIMIT
        ),
        cost_estimate=pl.CostEstimate(
            flops=2 * m * k * n, bytes_accessed=2 * (m * k + k * n + m * n), transcendentals=0
        ),
        name=name,
    )(a, b)


def solution(mesh):
    def step(x, dy, pre, w_in, w_down):
        d_pre, hidden_t, dy_all = front(dy, pre, w_down, mesh.shape["tp"])
        x, d_pre = lax.optimization_barrier((x, d_pre))
        x_all = lax.all_gather(x, axis_name="tp", axis=0, tiled=True)
        dx = lax.dot_general(
            d_pre, w_in, (((1,), (1,)), ((), ())), preferred_element_type=jnp.float32
        ).astype(jnp.bfloat16)
        hidden_t, dx = lax.optimization_barrier((hidden_t, dx))
        dx = lax.psum_scatter(dx, "tp", scatter_dimension=0, tiled=True)
        dw_down = weight_grad(hidden_t, dy_all, 512, False, "dw_down")
        d_pre, dw_down = lax.optimization_barrier((d_pre, dw_down))
        dw_in = weight_grad(x_all, d_pre, 512, True, "dw_in")
        return dx, dw_in, dw_down

    return jax.shard_map(
        step,
        mesh=mesh,
        in_specs=(
            P(("dp", "tp"), None),
            P(("dp", "tp"), None),
            P("dp", "tp"),
            P(None, "tp"),
            P("tp", None),
        ),
        out_specs=(P(("dp", "tp"), None), P("dp", "tp"), P(("dp", "tp"), None)),
        check_vma=False,
    )
```

```python
import functools

import jax
import jax.numpy as jnp
from jax import lax
from jax.experimental import pallas as pl
from jax.experimental.pallas import tpu as pltpu
from jax.sharding import PartitionSpec as P

MESH = pl.DeviceIdType.MESH
VMEM_LIMIT = 60 * 1024 * 1024


CHUNKS = 7
BLOCKS = 2
OUT = 512
PIECES = 4
STRIP = 256


def act(pre):
    return jax.nn.gelu(pre)


def front_kernel(
    dy_ref, pre_ref, w_ref, d_pre_ref, hidden_ref, all_ref,
    held, total, slope, pre_buf, hidden_buf, out_buf,
    send, recv, local, back, pre_sem, hidden_sem, out_sem,
):
    c, n = pl.program_id(0), pl.program_id(1)
    chunks, blocks = pl.num_programs(0), pl.num_programs(1)
    me = lax.axis_index("tp")
    right, left = lax.rem(me + 1, 4), lax.rem(me + 3, 4)
    rows, depth = dy_ref.shape[0], held.shape[2]
    half = rows // 2
    width = total.shape[2]
    per_block = width // STRIP
    strips = pre_ref.shape[1] // STRIP

    def columns(i, size):
        return pl.ds(pl.multiple_of(i * size, size), size)

    def rows_of(device, start, size):
        return pl.ds(pl.multiple_of(device * rows + start, 16), size)

    def load_own(i):
        return pltpu.make_async_copy(
            dy_ref.at[:, columns(i, depth)], held.at[i, rows_of(me, 0, rows), :], local.at[i]
        )

    def remote(kind, i, which, to):
        return pltpu.make_async_remote_copy(
            src_ref=held.at[i, which, :],
            dst_ref=held.at[i, which, :],
            send_sem=send.at[kind, i],
            recv_sem=recv.at[kind, i],
            device_id={"tp": to},
            device_id_type=MESH,
        )

    def own(i):
        which = rows_of(me, 0, rows)
        return remote(0, i, which, right), remote(1, i, which, left)

    def relay(i):
        return (
            remote(2, i, rows_of(left, 0, half), right),
            remote(3, i, rows_of(right, half, half), left),
        )

    def send_own(i):
        load_own(i).wait()
        for copy in own(i):
            copy.start()

    def pass_on(i):
        for arrived, onward in zip(own(i), relay(i)):
            arrived.wait_recv()
            onward.start()

    def load_pre(i, slot):
        return pltpu.make_async_copy(pre_ref.at[:, columns(i, STRIP)], pre_buf.at[slot], pre_sem.at[slot])

    def store_hidden(i, slot):
        return pltpu.make_async_copy(
            hidden_buf.at[slot], hidden_ref.at[columns(i, STRIP), :], hidden_sem.at[slot]
        )

    def gelu(i, _):
        slot = lax.rem(i, 2)
        load_pre(i, slot).wait()
        hidden, back_fn = jax.vjp(act, pre_buf[slot].astype(jnp.float32))
        at = (i // per_block, slice(None), columns(lax.rem(i, per_block), STRIP))
        slope[at] = back_fn(jnp.ones_like(hidden))[0]
        total[at] = jnp.zeros_like(hidden)

        @pl.when(i + 2 < strips)
        def _():
            load_pre(i + 2, slot).start()

        @pl.when(i >= 2)
        def _():
            store_hidden(i - 2, slot).wait()

        hidden_buf[slot] = hidden.astype(jnp.bfloat16).T
        store_hidden(i, slot).start()

    @pl.when((c == 0) & (n == 0))
    def _():
        for i in range(CHUNKS):
            load_own(i).start()
        for i in range(2):
            load_pre(i, i).start()
        barrier = pltpu.get_barrier_semaphore()
        for neighbour in (left, right):
            pl.semaphore_signal(barrier, inc=1, device_id={"tp": neighbour}, device_id_type=MESH)
        pl.semaphore_wait(barrier, 2)
        send_own(0)
        send_own(1)
        first, second = (strips * 9) // 16, (strips * 15) // 16
        lax.fori_loop(0, first, gelu, None)
        pass_on(0)
        send_own(2)
        lax.fori_loop(first, second, gelu, None)
        pass_on(1)
        send_own(3)
        lax.fori_loop(second, strips, gelu, None)
        for i in (strips - 2, strips - 1):
            store_hidden(i, i % 2).wait()

    @pl.when(n == 0)
    def _():
        for copy in relay(c):
            copy.wait_recv()
        pltpu.make_async_copy(held.at[c], all_ref.at[:, columns(c, depth)], back.at[c]).start()

    @pl.when((n == blocks - 1) & (c + 2 < chunks))
    def _():
        pass_on(c + 2)

        @pl.when(c + 4 < chunks)
        def _():
            send_own(c + 4)

    for s in range(width // OUT):
        cut = slice(s * OUT, (s + 1) * OUT)
        total[n, :, cut] += lax.dot_general(
            held[c], w_ref[cut, :], (((1,), (1,)), ((), ())), preferred_element_type=jnp.float32
        )

    stores = width // OUT

    def store_out(i):
        return pltpu.make_async_copy(out_buf, d_pre_ref.at[:, columns(i, OUT)], out_sem)

    @pl.when(c == chunks - 1)
    def _():
        for s in range(stores):
            i = n * stores + s
            at = (n, slice(None), slice(s * OUT, (s + 1) * OUT))

            @pl.when(i > 0)
            def _():
                store_out(i - 1).wait()

            out_buf[...] = (total[at] * slope[at]).astype(out_buf.dtype)
            store_out(i).start()

        @pl.when(n == blocks - 1)
        def _():
            store_out(n * stores + stores - 1).wait()
            for i in range(CHUNKS):
                pltpu.make_async_copy(held.at[i], all_ref.at[:, columns(i, depth)], back.at[i]).wait()
                for copy in own(i) + relay(i):
                    copy.wait_send()


def front(dy, pre, w, size):
    assert size == 4
    rows, d = pre.shape[0], dy.shape[1]
    f = w.shape[0]
    depth, width = d // CHUNKS, f // BLOCKS
    anywhere = pl.BlockSpec(memory_space=pl.ANY)
    bf16 = jnp.bfloat16
    return pl.pallas_call(
        front_kernel,
        grid=(CHUNKS, BLOCKS),
        in_specs=[anywhere, anywhere, pl.BlockSpec((width, depth), lambda c, n: (n, c))],
        out_specs=[anywhere] * 3,
        out_shape=[
            jax.ShapeDtypeStruct((rows, f), bf16),
            jax.ShapeDtypeStruct((f, rows), bf16),
            jax.ShapeDtypeStruct((rows, d), bf16),
        ],
        scratch_shapes=[
            pltpu.VMEM((CHUNKS, rows, depth), bf16),
            pltpu.VMEM((BLOCKS, rows, width), jnp.float32),
            pltpu.VMEM((BLOCKS, rows, width), jnp.float32),
            pltpu.VMEM((2, rows, STRIP), bf16),
            pltpu.VMEM((2, STRIP, rows), bf16),
            pltpu.VMEM((rows, OUT), bf16),
            pltpu.SemaphoreType.DMA((4, CHUNKS)),
            pltpu.SemaphoreType.DMA((4, CHUNKS)),
            pltpu.SemaphoreType.DMA((CHUNKS,)),
            pltpu.SemaphoreType.DMA((CHUNKS,)),
            pltpu.SemaphoreType.DMA((2,)),
            pltpu.SemaphoreType.DMA((2,)),
            pltpu.SemaphoreType.DMA,
        ],
        compiler_params=pltpu.CompilerParams(
            dimension_semantics=("arbitrary",) * 2,
            vmem_limit_bytes=67043328,
            collective_id=0,
            has_side_effects=True,
        ),
        cost_estimate=pl.CostEstimate(
            flops=2 * rows * f * d, bytes_accessed=2 * (f * d + 4 * rows * d), transcendentals=rows * f
        ),
        name="front",
    )(dy, pre, w)


def grad_kernel(transposed, a_ref, b_ref, out_ref, b_buf, out_buf, b_sem, out_sem):
    i, steps = pl.program_id(0), pl.num_programs(0)
    slot = lax.rem(i, 2)
    tile, n = out_buf.shape[1:]
    piece = n // PIECES
    dims = (((0,), (0,)), ((), ())) if transposed else (((1,), (0,)), ((), ()))

    def cut(q):
        return slice(q * piece, (q + 1) * piece)

    def load(q):
        return pltpu.make_async_copy(b_ref.at[:, cut(q)], b_buf.at[:, cut(q)], b_sem.at[q])

    def store(step, slot, q):
        rows = pl.ds(pl.multiple_of(step * tile, tile), tile)
        return pltpu.make_async_copy(
            out_buf.at[slot, :, cut(q)], out_ref.at[rows, cut(q)], out_sem.at[slot, q]
        )

    def product(columns):
        return lax.dot_general(
            a_ref[...], b_buf[:, columns], dims, preferred_element_type=jnp.float32
        ).astype(out_buf.dtype)

    @pl.when(i == 0)
    def _():
        for q in range(PIECES):
            load(q).start()

    @pl.when(i >= 2)
    def _():
        for q in range(PIECES):
            store(i - 2, slot, q).wait()

    edge = (i == 0) | (i == steps - 1)

    @pl.when(edge)
    def _():
        for q in range(PIECES):

            @pl.when(i == 0)
            def _():
                load(q).wait()

            out_buf[slot, :, cut(q)] = product(cut(q))
            store(i, slot, q).start()

    @pl.when(jnp.logical_not(edge))
    def _():
        out_buf[slot] = product(slice(None))
        for q in range(PIECES):
            store(i, slot, q).start()

    @pl.when(i == steps - 1)
    def _():
        for q in range(PIECES):
            store(i - 1, 1 - slot, q).wait()
        for q in range(PIECES):
            store(i, slot, q).wait()


def weight_grad(a, b, tile, transposed, name):
    k, n = b.shape
    m = a.shape[1] if transposed else a.shape[0]
    spec = (
        pl.BlockSpec((k, tile), lambda i: (0, i)) if transposed else pl.BlockSpec((tile, k), lambda i: (i, 0))
    )
    anywhere = pl.BlockSpec(memory_space=pl.ANY)
    return pl.pallas_call(
        functools.partial(grad_kernel, transposed),
        grid=(m // tile,),
        in_specs=[spec, anywhere],
        out_specs=anywhere,
        out_shape=jax.ShapeDtypeStruct((m, n), jnp.bfloat16),
        scratch_shapes=[
            pltpu.VMEM((k, n), jnp.bfloat16),
            pltpu.VMEM((2, tile, n), jnp.bfloat16),
            pltpu.SemaphoreType.DMA((PIECES,)),
            pltpu.SemaphoreType.DMA((2, PIECES)),
        ],
        compiler_params=pltpu.CompilerParams(
            dimension_semantics=("arbitrary",), vmem_limit_bytes=VMEM_LIMIT
        ),
        cost_estimate=pl.CostEstimate(
            flops=2 * m * k * n, bytes_accessed=2 * (m * k + k * n + m * n), transcendentals=0
        ),
        name=name,
    )(a, b)


def solution(mesh):
    def step(x, dy, pre, w_in, w_down):
        d_pre, hidden_t, dy_all = front(dy, pre, w_down, mesh.shape["tp"])
        x, d_pre = lax.optimization_barrier((x, d_pre))
        x_all = lax.all_gather(x, axis_name="tp", axis=0, tiled=True)
        dx = lax.dot_general(
            d_pre, w_in, (((1,), (1,)), ((), ())), preferred_element_type=jnp.float32
        ).astype(jnp.bfloat16)
        hidden_t, dx = lax.optimization_barrier((hidden_t, dx))
        dx = lax.psum_scatter(dx, "tp", scatter_dimension=0, tiled=True)
        dw_down = weight_grad(hidden_t, dy_all, 512, False, "dw_down")
        d_pre, dw_down = lax.optimization_barrier((d_pre, dw_down))
        dw_in = weight_grad(x_all, d_pre, 512, True, "dw_in")
        return dx, dw_in, dw_down

    return jax.shard_map(
        step,
        mesh=mesh,
        in_specs=(
            P(("dp", "tp"), None),
            P(("dp", "tp"), None),
            P("dp", "tp"),
            P(None, "tp"),
            P("tp", None),
        ),
        out_specs=(P(("dp", "tp"), None), P("dp", "tp"), P(("dp", "tp"), None)),
        check_vma=False,
    )
```

```python
import functools

import jax
import jax.numpy as jnp
from jax import lax
from jax.experimental import pallas as pl
from jax.experimental.pallas import tpu as pltpu
from jax.sharding import PartitionSpec as P

MESH = pl.DeviceIdType.MESH
VMEM_LIMIT = 60 * 1024 * 1024


CHUNKS = 7
BLOCKS = 4
STRIP = 256


def act(pre):
    return jax.nn.gelu(pre)


def whole(shape):
    return pl.BlockSpec(shape, lambda *i: (0,) * len(shape), pipeline_mode=pl.Buffered(1))


def front_kernel(
    dy_ref, pre_ref, w_ref, d_pre_ref, hidden_ref, all_ref,
    held, total, slope, pre_buf, hidden_buf, out_buf,
    send, recv, local, back, pre_sem, hidden_sem, out_sem,
):
    c, n = pl.program_id(0), pl.program_id(1)
    chunks, blocks = pl.num_programs(0), pl.num_programs(1)
    me = lax.axis_index("tp")
    right, left = lax.rem(me + 1, 4), lax.rem(me + 3, 4)
    rows, depth = dy_ref.shape[0], held.shape[2]
    half = rows // 2
    width = total.shape[2]
    per_block = width // STRIP
    strips = pre_ref.shape[1] // STRIP

    def columns(i, size):
        return pl.ds(pl.multiple_of(i * size, size), size)

    def rows_of(device, start, size):
        return pl.ds(pl.multiple_of(device * rows + start, 16), size)

    def load_own(i):
        return pltpu.make_async_copy(
            dy_ref.at[:, columns(i, depth)], held.at[i, rows_of(me, 0, rows), :], local.at[i]
        )

    def remote(kind, i, which, to):
        return pltpu.make_async_remote_copy(
            src_ref=held.at[i, which, :],
            dst_ref=held.at[i, which, :],
            send_sem=send.at[kind, i],
            recv_sem=recv.at[kind, i],
            device_id={"tp": to},
            device_id_type=MESH,
        )

    def first(i):
        return remote(0, i, rows_of(me, 0, half), right), remote(1, i, rows_of(me, half, half), left)

    def rest(i):
        return remote(4, i, rows_of(me, half, half), right), remote(5, i, rows_of(me, 0, half), left)

    def relay(i):
        return (
            remote(2, i, rows_of(left, 0, half), right),
            remote(3, i, rows_of(right, half, half), left),
        )

    def send_first(i):
        load_own(i).wait()
        for copy in first(i):
            copy.start()

    def send_rest(i):
        for copy in rest(i):
            copy.start()

    def pass_on(i):
        for arrived, onward in zip(first(i), relay(i)):
            arrived.wait_recv()
            onward.start()

    def load_pre(i, slot):
        return pltpu.make_async_copy(pre_ref.at[:, columns(i, STRIP)], pre_buf.at[slot], pre_sem.at[slot])

    def store_hidden(i, slot):
        return pltpu.make_async_copy(
            hidden_buf.at[slot], hidden_ref.at[columns(i, STRIP), :], hidden_sem.at[slot]
        )

    def gelu(i, _):
        slot = lax.rem(i, 2)
        load_pre(i, slot).wait()
        hidden, back_fn = jax.vjp(act, pre_buf[slot].astype(jnp.float32))
        at = (i // per_block, slice(None), columns(lax.rem(i, per_block), STRIP))
        slope[at] = back_fn(jnp.ones_like(hidden))[0]
        total[at] = jnp.zeros_like(hidden)

        @pl.when(i + 2 < strips)
        def _():
            load_pre(i + 2, slot).start()

        @pl.when(i >= 2)
        def _():
            store_hidden(i - 2, slot).wait()

        hidden_buf[slot] = hidden.astype(jnp.bfloat16).T
        store_hidden(i, slot).start()

    @pl.when((c == 0) & (n == 0))
    def _():
        for i in range(CHUNKS):
            load_own(i).start()
        for i in range(2):
            load_pre(i, i).start()
        barrier = pltpu.get_barrier_semaphore()
        for neighbour in (left, right):
            pl.semaphore_signal(barrier, inc=1, device_id={"tp": neighbour}, device_id_type=MESH)
        pl.semaphore_wait(barrier, 2)
        send_first(0)
        send_rest(0)
        send_first(1)
        one, two = (strips * 5) // 14, (strips * 11) // 14
        lax.fori_loop(0, one, gelu, None)
        pass_on(0)
        send_rest(1)
        send_first(2)
        lax.fori_loop(one, two, gelu, None)
        pass_on(1)
        send_rest(2)
        send_first(3)
        lax.fori_loop(two, strips, gelu, None)
        for i in (strips - 2, strips - 1):
            store_hidden(i, i % 2).wait()

    @pl.when(n == 0)
    def _():
        for copy in relay(c) + rest(c):
            copy.wait_recv()
        pltpu.make_async_copy(held.at[c], all_ref.at[:, columns(c, depth)], back.at[c]).start()

    @pl.when((n == blocks - 1) & (c + 2 < chunks))
    def _():
        pass_on(c + 2)

        @pl.when(c + 3 < chunks)
        def _():
            send_rest(c + 3)

        @pl.when(c + 4 < chunks)
        def _():
            send_first(c + 4)

    def product():
        return lax.dot_general(
            held[c], w_ref[...], (((1,), (1,)), ((), ())), preferred_element_type=jnp.float32
        )

    @pl.when(c < chunks - 1)
    def _():
        total[n] += product()

    def store_out(i):
        return pltpu.make_async_copy(out_buf, d_pre_ref.at[:, columns(i, width)], out_sem)

    @pl.when(c == chunks - 1)
    def _():
        @pl.when(n > 0)
        def _():
            store_out(n - 1).wait()

        out_buf[...] = ((total[n] + product()) * slope[n]).astype(out_buf.dtype)
        store_out(n).start()

        @pl.when(n == blocks - 1)
        def _():
            store_out(n).wait()
            for i in range(CHUNKS):
                pltpu.make_async_copy(held.at[i], all_ref.at[:, columns(i, depth)], back.at[i]).wait()
                for copy in first(i) + relay(i) + rest(i):
                    copy.wait_send()


def front(dy, pre, w, size):
    assert size == 4
    rows, d = pre.shape[0], dy.shape[1]
    f = w.shape[0]
    depth, width = d // CHUNKS, f // BLOCKS
    anywhere = pl.BlockSpec(memory_space=pl.ANY)
    bf16 = jnp.bfloat16
    return pl.pallas_call(
        front_kernel,
        grid=(CHUNKS, BLOCKS),
        in_specs=[anywhere, anywhere, pl.BlockSpec((width, depth), lambda c, n: (n, c))],
        out_specs=[anywhere] * 3,
        out_shape=[
            jax.ShapeDtypeStruct((rows, f), bf16),
            jax.ShapeDtypeStruct((f, rows), bf16),
            jax.ShapeDtypeStruct((rows, d), bf16),
        ],
        scratch_shapes=[
            pltpu.VMEM((CHUNKS, rows, depth), bf16),
            pltpu.VMEM((BLOCKS, rows, width), jnp.float32),
            pltpu.VMEM((BLOCKS, rows, width), jnp.float32),
            pltpu.VMEM((2, rows, STRIP), bf16),
            pltpu.VMEM((2, STRIP, rows), bf16),
            pltpu.VMEM((rows, width), bf16),
            pltpu.SemaphoreType.DMA((6, CHUNKS)),
            pltpu.SemaphoreType.DMA((6, CHUNKS)),
            pltpu.SemaphoreType.DMA((CHUNKS,)),
            pltpu.SemaphoreType.DMA((CHUNKS,)),
            pltpu.SemaphoreType.DMA((2,)),
            pltpu.SemaphoreType.DMA((2,)),
            pltpu.SemaphoreType.DMA,
        ],
        compiler_params=pltpu.CompilerParams(
            dimension_semantics=("arbitrary",) * 2,
            vmem_limit_bytes=67043328,
            collective_id=0,
            has_side_effects=True,
        ),
        cost_estimate=pl.CostEstimate(
            flops=2 * rows * f * d, bytes_accessed=2 * (f * d + 4 * rows * d), transcendentals=rows * f
        ),
        name="front",
    )(dy, pre, w)


def product_kernel(a_ref, b_ref, out_ref):
    out_ref[...] = jnp.dot(a_ref[...], b_ref[...], preferred_element_type=jnp.float32).astype(out_ref.dtype)


def product_t_kernel(a_ref, b_ref, out_ref):
    out_ref[...] = lax.dot_general(
        a_ref[...], b_ref[...], (((0,), (0,)), ((), ())), preferred_element_type=jnp.float32
    ).astype(out_ref.dtype)


def weight_grad(a, b, tile, transposed, name):
    k, n = b.shape
    m = a.shape[1] if transposed else a.shape[0]
    spec = (
        pl.BlockSpec((k, tile), lambda i: (0, i)) if transposed else pl.BlockSpec((tile, k), lambda i: (i, 0))
    )
    return pl.pallas_call(
        product_t_kernel if transposed else product_kernel,
        grid=(m // tile,),
        in_specs=[spec, whole((k, n))],
        out_specs=pl.BlockSpec((tile, n), lambda i: (i, 0)),
        out_shape=jax.ShapeDtypeStruct((m, n), jnp.bfloat16),
        compiler_params=pltpu.CompilerParams(
            dimension_semantics=("arbitrary",), vmem_limit_bytes=VMEM_LIMIT
        ),
        cost_estimate=pl.CostEstimate(
            flops=2 * m * k * n, bytes_accessed=2 * (m * k + k * n + m * n), transcendentals=0
        ),
        name=name,
    )(a, b)


def solution(mesh):
    def step(x, dy, pre, w_in, w_down):
        d_pre, hidden_t, dy_all = front(dy, pre, w_down, mesh.shape["tp"])
        x, d_pre = lax.optimization_barrier((x, d_pre))
        x_all = lax.all_gather(x, axis_name="tp", axis=0, tiled=True)
        dx = lax.dot_general(
            d_pre, w_in, (((1,), (1,)), ((), ())), preferred_element_type=jnp.float32
        ).astype(jnp.bfloat16)
        hidden_t, dx = lax.optimization_barrier((hidden_t, dx))
        dx = lax.psum_scatter(dx, "tp", scatter_dimension=0, tiled=True)
        dw_down = weight_grad(hidden_t, dy_all, 512, False, "dw_down")
        d_pre, dw_down = lax.optimization_barrier((d_pre, dw_down))
        dw_in = weight_grad(x_all, d_pre, 512, True, "dw_in")
        return dx, dw_in, dw_down

    return jax.shard_map(
        step,
        mesh=mesh,
        in_specs=(
            P(("dp", "tp"), None),
            P(("dp", "tp"), None),
            P("dp", "tp"),
            P(None, "tp"),
            P("tp", None),
        ),
        out_specs=(P(("dp", "tp"), None), P("dp", "tp"), P(("dp", "tp"), None)),
        check_vma=False,
    )
```
